32 devices in a mesh: fsdp: 2 (over core), width: 4 (over y, x), unit: 4 (over z).
Axes of the slice: x: 2, y: 2, z: 4, core: 2. Of those that a mesh axis runs over, the one named last changes fastest.
Arguments:
- train_gate: bfloat16 [8192, 8192], P(('unit', 'fsdp'), 'width'), parts along dimension 0, may hold values from -0.125 to 0.125
- low_gate: bfloat16 [8192, 32], P(('unit', 'fsdp')), parts along dimension 0, may hold values from -0.125 to 0.125
- high_gate: bfloat16 [128, 8192], P('unit', 'width'), parts along dimension 0, may hold values from -1 to 1
- train_up: bfloat16 [8192, 8192], P(('unit', 'fsdp'), 'width'), parts along dimension 0, may hold values from -0.125 to 0.125
- low_up: bfloat16 [8192, 32], P(('unit', 'fsdp')), parts along dimension 0, may hold values from -0.125 to 0.125
- high_up: bfloat16 [128, 8192], P('unit', 'width'), parts along dimension 0, may hold values from -1 to 1
- norm_train: float32 [8192], P(('unit', 'fsdp', 'width')), parts along dimension 0, may hold values from 0.25 to 1.75
- norm_step: float32 [8192], P(('unit', 'fsdp', 'width')), parts along dimension 0, may hold values from -0.3 to 0.3
Outputs:
- final_gate: bfloat16 [32768, 2048], P(('unit', 'width')), parts along dimension 0
- final_up: bfloat16 [32768, 2048], P(('unit', 'width')), parts along dimension 0
- serve_norm: bfloat16 [8192], P('unit'), parts along dimension 0
The draws below stay inside these ranges and needn't reach their ends.
There are 4 independent parts, one for each index of `unit`. The reference program is written for one: setup_inputs(seed, part) draws one part's arguments, and reference() takes and returns one part's arrays. A program takes and returns all parts, laid end to end along the dimension named above; each array names one. Nothing has to cross between parts.
All inputs are finite; a program needn't handle non-finite values.
Results may differ from the reference program's by a relative error of at most 0.001.
Values may be sent and summed in bfloat16 or wider, within the bound.
A program may use at most 128 MiB of HBM per device.

```python
import jax
import jax.numpy as jnp

D_MODEL = 2048
D_INNER = 8192
RANK = 32


def block_levels(key, dims, pieces, least, high):
    factor_of = 1.0
    for axis_at, shards_of in pieces:
        steps = jax.random.uniform(jax.random.fold_in(jax.random.fold_in(key, 6), axis_at), (shards_of,), jnp.float32, least / len(pieces), high / len(pieces))
        factor_of = factor_of * jnp.repeat(jnp.exp(steps), dims[axis_at] // shards_of).reshape((-1,) + (1,) * (len(dims) - 1 - axis_at))
    return factor_of


def centred(own_key, extent, scale, reach, cuts=(), kind=jnp.bfloat16):
    values = scale * jax.random.normal(own_key, extent, jnp.float32)
    if cuts:
        values = values * block_levels(own_key, extent, cuts, -0.22, 0.18)
    return jnp.clip(values, -reach, reach).astype(kind)


def setup_inputs(seed: int = 0, part: int = 0) -> dict:
    streams_of = jax.random.split(jax.random.key(seed), 9)
    own_keys = jax.random.split(jax.random.fold_in(streams_of[8], part), 9)
    train_gate = centred(own_keys[0], (D_MODEL, D_INNER), D_MODEL ** -0.5, 0.125, ((0, 2), (1, 4)))
    low_gate = centred(own_keys[1], (D_MODEL, RANK), D_MODEL ** -0.5, 0.125, ((0, 2),))
    high_gate = centred(own_keys[2], (RANK, D_INNER), RANK ** -0.5, 1.0, ((1, 4),))
    train_up = centred(own_keys[3], (D_MODEL, D_INNER), D_MODEL ** -0.5, 0.125, ((0, 2), (1, 4)))
    low_up = centred(own_keys[4], (D_MODEL, RANK), D_MODEL ** -0.5, 0.125, ((0, 2),))
    high_up = centred(own_keys[5], (RANK, D_INNER), RANK ** -0.5, 1.0, ((1, 4),))
    norm_train = jnp.clip(1.0 + 0.15 * jax.random.normal(own_keys[6], (D_MODEL,), jnp.float32), 0.25, 1.75)
    norm_step = jnp.clip(jax.random.uniform(own_keys[7], (D_MODEL,), jnp.float32, -0.3, 0.3) * block_levels(own_keys[7], (D_MODEL,), ((0, 8),), -0.4, 0.0), -0.3, 0.3)
    return dict(train_gate=train_gate, low_gate=low_gate, high_gate=high_gate, train_up=train_up, low_up=low_up, high_up=high_up, norm_train=norm_train, norm_step=norm_step)


mix_rate = 2.0


def reference(train_gate, low_gate, high_gate, train_up, low_up, high_up, norm_train, norm_step):
    result_gate = train_gate.astype(jnp.float32) + mix_rate * jnp.dot(low_gate, high_gate, preferred_element_type=jnp.float32)
    result_up = train_up.astype(jnp.float32) + mix_rate * jnp.dot(low_up, high_up, preferred_element_type=jnp.float32)
    final_gate = result_gate.T.astype(jnp.bfloat16)
    final_up = result_up.T.astype(jnp.bfloat16)
    serve_norm = (norm_train + norm_step).astype(jnp.bfloat16)
    return final_gate, final_up, serve_norm
```

```python
import functools

import jax
import jax.numpy as jnp
from jax import lax
from jax.experimental import pallas as pl
from jax.experimental.pallas import tpu as pltpu
from jax.sharding import PartitionSpec as P

mix_rate = 2.0


def piece_kernel(at_ref, train_ref, low_ref, high_ref, *rest):
    out_ref = rest[-1]
    width = train_ref.shape[1]
    high = (high_ref[...].astype(jnp.float32) * mix_rate).astype(jnp.bfloat16)
    mixed = lax.dot_general(
        high, low_ref[...], (((0,), (0,)), ((), ())), preferred_element_type=jnp.float32
    )
    out_ref[...] = (train_ref[...].T.astype(jnp.float32) + mixed).astype(out_ref.dtype)


def place_piece(at, train, low, high, whole, total):
    rows, columns = train.shape
    rank = high.shape[0]
    block = min(512, columns)
    in_specs = [
        pl.BlockSpec((rows, block), lambda i, at: (0, i)),
        pl.BlockSpec((rank, rows), lambda i, at: (0, 0)),
        pl.BlockSpec((rank, block), lambda i, at: (0, i)),
    ]
    operands = [train, low, high]
    aliases = {}
    if whole is not None:
        in_specs.append(pl.BlockSpec(memory_space=pl.ANY))
        operands.append(whole)
        aliases = {4: 0}
    return pl.pallas_call(
        piece_kernel,
        out_shape=jax.ShapeDtypeStruct((columns, total), jnp.bfloat16),
        grid_spec=pltpu.PrefetchScalarGridSpec(
            num_scalar_prefetch=1,
            grid=(columns // block,),
            in_specs=in_specs,
            out_specs=pl.BlockSpec((block, rows), lambda i, at: (i, at[0])),
        ),
        input_output_aliases=aliases,
        compiler_params=pltpu.CompilerParams(dimension_semantics=("arbitrary",)),
        cost_estimate=pl.CostEstimate(
            flops=2 * rows * columns * rank, bytes_accessed=4 * rows * columns, transcendentals=0
        ),
    )(at, *operands)


def gain_kernel(sizes, mine_ref, all_ref, send_sem, recv_sem, own_sem):
    fsdp, width = sizes
    count = fsdp * width
    row, column = lax.axis_index("fsdp"), lax.axis_index("width")
    me = row * width + column

    def peer(step):
        to = lax.rem(me + step, count)
        return {"fsdp": to // width, "width": lax.rem(to, width)}

    barrier = pltpu.get_barrier_semaphore()
    for step in range(1, count):
        pl.semaphore_signal(barrier, inc=1, device_id=peer(step))
    own = pltpu.make_async_copy(mine_ref, all_ref.at[me], own_sem)
    own.start()
    pl.semaphore_wait(barrier, count - 1)
    copies = []
    for step in range(1, count):
        copy = pltpu.make_async_remote_copy(
            src_ref=mine_ref,
            dst_ref=all_ref.at[me],
            send_sem=send_sem.at[step],
            recv_sem=recv_sem.at[step],
            device_id=peer(step),
        )
        copy.start()
        copies.append(copy)
    own.wait()
    for copy in copies:
        copy.wait()


def gather_gain(gain, sizes):
    count = sizes[0] * sizes[1]
    shape = (gain.shape[0] // 128, 128) if gain.shape[0] % 128 == 0 else (1, gain.shape[0])
    gathered = pl.pallas_call(
        functools.partial(gain_kernel, sizes),
        out_shape=jax.ShapeDtypeStruct((count,) + shape, jnp.float32),
        in_specs=[pl.BlockSpec(memory_space=pltpu.VMEM)],
        out_specs=pl.BlockSpec(memory_space=pltpu.VMEM),
        scratch_shapes=[
            pltpu.SemaphoreType.DMA((count,)),
            pltpu.SemaphoreType.DMA((count,)),
            pltpu.SemaphoreType.DMA,
        ],
        compiler_params=pltpu.CompilerParams(collective_id=0, has_side_effects=True),
        cost_estimate=pl.CostEstimate(flops=0, bytes_accessed=8000000, transcendentals=0),
    )(gain.reshape(shape))
    return gathered.reshape(-1).astype(jnp.bfloat16)


def solution(mesh):
    fsdp, width = mesh.shape["fsdp"], mesh.shape["width"]

    def body(train_gate, low_gate, high_gate, train_up, low_up, high_up, norm_train, norm_step):
        total = train_gate.shape[0] * fsdp
        me = lax.axis_index("fsdp").astype(jnp.int32)
        lows = (low_gate.T, low_up.T)
        trains = (train_gate, train_up)
        highs = (high_gate, high_up)
        arrived = []
        for step in range(1, fsdp):
            ring = [(at, (at + step) % fsdp) for at in range(fsdp)]
            for which in range(2):
                arrived.append(
                    (
                        which,
                        lax.rem(me + fsdp - step, fsdp),
                        lax.ppermute(lows[which], "fsdp", ring),
                        lax.ppermute(trains[which], "fsdp", ring),
                    )
                )
        finals = [
            place_piece(me.reshape(1), trains[which], lows[which], highs[which], None, total)
            for which in range(2)
        ]
        serve_norm = gather_gain(norm_train + norm_step, (fsdp, width))
        for which, at, low, train in arrived:
            finals[which] = place_piece(
                at.reshape(1), train, low, highs[which], finals[which], total
            )
        return (finals[0], finals[1], serve_norm)

    return jax.shard_map(
        body,
        mesh=mesh,
        in_specs=(
            P(("unit", "fsdp"), "width"),
            P(("unit", "fsdp"), None),
            P("unit", "width"),
            P(("unit", "fsdp"), "width"),
            P(("unit", "fsdp"), None),
            P("unit", "width"),
            P(("unit", "fsdp", "width")),
            P(("unit", "fsdp", "width")),
        ),
        out_specs=(P(("unit", "width"), None), P(("unit", "width"), None), P("unit")),
        check_vma=False,
    )
```

```python
import functools

import jax
import jax.numpy as jnp
from jax import lax
from jax.experimental import pallas as pl
from jax.experimental.pallas import tpu as pltpu
from jax.sharding import PartitionSpec as P

mix_rate = 2.0
grant = 60 * 1024 * 1024


def piece_kernel(count, rows, columns, block, gain_too, at_ref, *refs):
    trains, lows, highs = refs[:count], refs[count : 2 * count], refs[2 * count : 3 * count]
    rest = refs[3 * count :]
    gains = None
    if gain_too:
        gains, rest = rest[0], rest[1:]
    scratch = rest[-8:]
    outs = rest[-8 - count - gain_too : -8]
    train_buf, low_buf, high_buf, out_buf, train_sem, low_sem, high_sem, out_sem = scratch
    chunks = columns // block
    first = pl.multiple_of(at_ref[0] * rows, rows)

    small, loads = [], []
    for which in range(count):
        small.append(
            (
                pltpu.make_async_copy(lows[which], low_buf.at[which], low_sem.at[which]),
                pltpu.make_async_copy(highs[which], high_buf.at[which], high_sem.at[which]),
            )
        )
        loads.append(
            [
                pltpu.make_async_copy(
                    trains[which].at[:, pl.ds(chunk * block, block)],
                    train_buf.at[which * chunks + chunk],
                    train_sem.at[which * chunks + chunk],
                )
                for chunk in range(chunks)
            ]
        )
    for which in range(count):
        for copy in small[which]:
            copy.start()
        for copy in loads[which]:
            copy.start()
    if gain_too:
        outs[count][...] = (gains[:, 0] + gains[:, 1]).astype(outs[count].dtype)
    stores = []
    for which in range(count):
        for copy in small[which]:
            copy.wait()
        low = low_buf[which]
        for chunk in range(chunks):
            slot = which * chunks + chunk
            high = high_buf[which, :, pl.ds(chunk * block, block)].astype(jnp.float32) * mix_rate
            mixed = lax.dot_general(
                high.astype(jnp.bfloat16),
                low,
                (((0,), (0,)), ((), ())),
                preferred_element_type=jnp.float32,
            )
            loads[which][chunk].wait()
            out_buf[slot] = (train_buf[slot].T.astype(jnp.float32) + mixed).astype(jnp.bfloat16)
            store = pltpu.make_async_copy(
                out_buf.at[slot],
                outs[which].at[pl.ds(chunk * block, block), pl.ds(first, rows)],
                out_sem.at[slot],
            )
            store.start()
            stores.append(store)
    for store in stores:
        store.wait()


def place_pieces(at, trains, lows, highs, wholes, total, gains=None):
    count = len(trains)
    rows, columns = trains[0].shape
    rank = highs[0].shape[0]
    block = min(256, columns)
    slots = count * (columns // block)
    anywhere = pl.BlockSpec(memory_space=pl.ANY)
    operands = [at, *trains, *lows, *highs]
    in_specs = [pl.BlockSpec(memory_space=pltpu.SMEM)] + [anywhere] * (3 * count)
    out_shape = [jax.ShapeDtypeStruct((columns, total), jnp.bfloat16)] * count
    out_specs = [anywhere] * count
    aliases = {}
    if gains is not None:
        operands.append(gains)
        in_specs.append(pl.BlockSpec(memory_space=pltpu.VMEM))
        out_shape.append(
            jax.ShapeDtypeStruct(gains.shape[:1] + gains.shape[2:], jnp.bfloat16)
        )
        out_specs.append(pl.BlockSpec(memory_space=pltpu.VMEM))
    if wholes is not None:
        aliases = {len(operands) + which: which for which in range(count)}
        operands += wholes
        in_specs += [anywhere] * count
    return pl.pallas_call(
        functools.partial(piece_kernel, count, rows, columns, block, int(gains is not None)),
        out_shape=out_shape,
        in_specs=in_specs,
        out_specs=out_specs,
        input_output_aliases=aliases,
        scratch_shapes=[
            pltpu.VMEM((slots, rows, block), jnp.bfloat16),
            pltpu.VMEM((count, rank, rows), jnp.bfloat16),
            pltpu.VMEM((count, rank, columns), jnp.bfloat16),
            pltpu.VMEM((slots, block, rows), jnp.bfloat16),
            pltpu.SemaphoreType.DMA((slots,)),
            pltpu.SemaphoreType.DMA((count,)),
            pltpu.SemaphoreType.DMA((count,)),
            pltpu.SemaphoreType.DMA((slots,)),
        ],
        compiler_params=pltpu.CompilerParams(vmem_limit_bytes=grant),
        cost_estimate=pl.CostEstimate(
            flops=2 * count * rows * columns * rank,
            bytes_accessed=4 * count * rows * columns,
            transcendentals=0,
        ),
    )(*operands)


def gain_kernel(sizes, train_ref, step_ref, after_ref, all_ref, send_sem, recv_sem, own_sem):
    fsdp, width = sizes
    count = fsdp * width
    row, column = lax.axis_index("fsdp"), lax.axis_index("width")
    me = row * width + column
    parts = (train_ref, step_ref)

    def peer(step):
        to = lax.rem(me + step, count)
        return {"fsdp": to // width, "width": lax.rem(to, width)}

    barrier = pltpu.get_barrier_semaphore()
    for step in range(1, count):
        pl.semaphore_signal(barrier, inc=1, device_id=peer(step))
    owns = [
        pltpu.make_async_copy(part, all_ref.at[me, kind], own_sem.at[kind])
        for kind, part in enumerate(parts)
    ]
    for own in owns:
        own.start()
    pl.semaphore_wait(barrier, count - 1)
    copies = []
    for step in range(1, count):
        for kind, part in enumerate(parts):
            copy = pltpu.make_async_remote_copy(
                src_ref=part,
                dst_ref=all_ref.at[me, kind],
                send_sem=send_sem.at[step, kind],
                recv_sem=recv_sem.at[step, kind],
                device_id=peer(step),
            )
            copy.start()
            copies.append(copy)
    for own in owns:
        own.wait()
    for copy in copies:
        copy.wait()


def gather_gains(norm_train, norm_step, sizes, after):
    count = sizes[0] * sizes[1]
    extent = norm_train.shape[0]
    shape = (extent // 128, 128) if extent % 128 == 0 else (1, extent)
    return pl.pallas_call(
        functools.partial(gain_kernel, sizes),
        out_shape=jax.ShapeDtypeStruct((count, 2) + shape, jnp.float32),
        in_specs=[
            pl.BlockSpec(memory_space=pltpu.VMEM),
            pl.BlockSpec(memory_space=pltpu.VMEM),
            pl.BlockSpec(memory_space=pl.ANY),
        ],
        out_specs=pl.BlockSpec(memory_space=pltpu.VMEM),
        scratch_shapes=[
            pltpu.SemaphoreType.DMA((count, 2)),
            pltpu.SemaphoreType.DMA((count, 2)),
            pltpu.SemaphoreType.DMA((2,)),
        ],
        compiler_params=pltpu.CompilerParams(
            collective_id=0, has_side_effects=True, vmem_limit_bytes=grant
        ),
        cost_estimate=pl.CostEstimate(flops=0, bytes_accessed=8000000, transcendentals=0),
    )(norm_train.reshape(shape), norm_step.reshape(shape), after)


def solution(mesh):
    fsdp, width = mesh.shape["fsdp"], mesh.shape["width"]

    def body(train_gate, low_gate, high_gate, train_up, low_up, high_up, norm_train, norm_step):
        total = train_gate.shape[0] * fsdp
        me = lax.axis_index("fsdp").astype(jnp.int32)
        lows = (low_gate.T, low_up.T)
        trains = (train_gate, train_up)
        highs = (high_gate, high_up)
        arrived = []
        for step in range(1, fsdp):
            ring = [(at, (at + step) % fsdp) for at in range(fsdp)]
            for which in range(2):
                arrived.append(
                    (
                        which,
                        lax.rem(me + fsdp - step, fsdp),
                        lax.ppermute(lows[which], "fsdp", ring),
                        lax.ppermute(trains[which], "fsdp", ring),
                    )
                )
        finals = list(place_pieces(me.reshape(1), trains, lows, highs, None, total))
        for which, at, low, train in arrived[:-1]:
            (finals[which],) = place_pieces(
                at.reshape(1), [train], [low], [highs[which]], [finals[which]], total
            )
        gains = gather_gains(norm_train, norm_step, (fsdp, width), finals[0])
        which, at, low, train = arrived[-1]
        finals[which], serve_norm = place_pieces(
            at.reshape(1), [train], [low], [highs[which]], [finals[which]], total, gains
        )
        serve_norm = serve_norm.reshape(-1)
        return (finals[0], finals[1], serve_norm)

    return jax.shard_map(
        body,
        mesh=mesh,
        in_specs=(
            P(("unit", "fsdp"), "width"),
            P(("unit", "fsdp"), None),
            P("unit", "width"),
            P(("unit", "fsdp"), "width"),
            P(("unit", "fsdp"), None),
            P("unit", "width"),
            P(("unit", "fsdp", "width")),
            P(("unit", "fsdp", "width")),
        ),
        out_specs=(P(("unit", "width"), None), P(("unit", "width"), None), P("unit")),
        check_vma=False,
    )
```
